128 devices in a mesh: grp: 4 (over z), tile: 32 (over x, y, core).
Axes of the slice: x: 4, y: 4, z: 4, core: 2. Of those that a mesh axis runs over, the one named last changes fastest.
Arguments:
- noise: bfloat16 [16, 3, 2048, 2048], P('grp', None, 'tile'), may hold values from -6 to 6
- stress: float32 [6, 2048, 2048], P(None, 'tile', 'grp'), as said below
- timescale: float32 [2048, 2048], P('tile', 'grp'), may hold values from 3 to 256
- mean_inflow: float32 [2048, 2048], P('tile', 'grp'), may hold values from 0.5 to 1.5
- courant: float32 [2048, 2048], P('tile', 'grp'), may hold values from 0.2 to 0.9
- prior_state: float32 [3, 2048, 2048], P(None, 'tile', 'grp'), may hold values from -6 to 6
- field: float32 [3, 8, 2048, 2048], P(None, None, 'tile', 'grp'), may hold values from -6 to 6
Outputs:
- inflow: bfloat16 [16, 3, 2048, 2048], P(None, None, 'tile', 'grp')
- field_out: float32 [3, 8, 2048, 2048], P(None, None, 'tile', 'grp')
The draws below stay inside these ranges and needn't reach their ends.
Inputs may be any that keep to these rules, and one draw needn't show every extreme that they name: stress holds, per cell, R11, R21, R22, R31, R32, R33 of a symmetric positive definite tensor whose Cholesky factor has diagonal entries of 0.3 or more.
All inputs are finite; a program needn't handle non-finite values.
Results may differ from the reference program's by a relative error of at most 0.0085.
Values may be sent and summed in bfloat16 or wider, within the bound.
A program may use at most 128 MiB of HBM per device.

```python
import math
import jax
import jax.numpy as jnp
from jax import lax

NY = 2048
NZ = 2048
LS = 2
FW = 4
CX = 8
PLANES = 16


def draw_stress(key, part):
    diag_key = jax.random.fold_in(key, 11)
    lower_key = jax.random.fold_in(key, 23)
    smallest, largest, reach = (0.3, 1.5, 0.6)
    diagonal = jnp.exp(jax.random.uniform(diag_key, (3, NZ, NY), jnp.float32, math.log(smallest), math.log(largest)))
    lower = jax.random.uniform(lower_key, (3, NZ, NY), jnp.float32, -reach, reach)
    first_diag, second_diag, third_diag = (diagonal[0], diagonal[1], diagonal[2])
    second_low, third_low, third_mid = (lower[0], lower[1], lower[2])
    return jnp.stack([first_diag * first_diag, second_low * first_diag, second_low * second_low + second_diag * second_diag, third_low * first_diag, third_low * second_low + third_mid * second_diag, third_low * third_low + third_mid * third_mid + third_diag * third_diag]).astype(jnp.float32)


def block_scale(key, dims, cuts, low, high):
    loudness, own = 1.0, jax.random.fold_in(key, 6)
    for dim, shards_of in cuts:
        heights = jnp.exp(jax.random.uniform(jax.random.fold_in(own, dim), (shards_of,), jnp.float32, low / len(cuts), high / len(cuts)))
        loudness = loudness * jnp.repeat(heights, dims[dim] // shards_of).reshape([-1 if axis == dim else 1 for axis in range(len(dims))])
    return loudness


def normal_values(own_key, extent, spread, bound, split=(), held_as=jnp.bfloat16):
    result = spread * jax.random.normal(own_key, extent, jnp.float32)
    if split:
        result = result * block_scale(own_key, extent, split, -0.22, 0.18)
    return jnp.clip(result, -bound, bound).astype(held_as)


def setup_inputs(seed: int = 0) -> dict:
    key_of = jax.random.split(jax.random.key(seed), 8)
    noise = normal_values(key_of[0], (PLANES, 3, NY, NZ), 1.0, 6.0, ((0, 4), (2, 32)))
    stress = draw_stress(jax.random.fold_in(key_of[7], 71), 0)
    timescale = jnp.clip(jnp.exp(math.log(256.0) - 4.446565 * jax.random.uniform(key_of[2], (NZ, NY), jnp.float32) ** block_scale(key_of[2], (NZ, NY), ((0, 32), (1, 4)), -0.2, 0.2)), 3.0, 256.0)
    mean_inflow = jnp.clip(0.5 + 1.0 * jax.random.uniform(key_of[3], (NZ, NY), jnp.float32) ** block_scale(key_of[3], (NZ, NY), ((0, 32), (1, 4)), -0.2, 0.2), 0.5, 1.5)
    courant = jnp.clip(jnp.exp(math.log(0.9) - 1.50407736 * jax.random.uniform(key_of[4], (NZ, NY), jnp.float32) ** block_scale(key_of[4], (NZ, NY), ((0, 32), (1, 4)), -0.2, 0.2)), 0.2, 0.9)
    prior_state = normal_values(key_of[5], (3, NZ, NY), 1.0, 6.0, ((1, 32), (2, 4)), jnp.float32)
    field = normal_values(key_of[6], (3, CX, NZ, NY), 1.0, 6.0, ((2, 32), (3, 4)), jnp.float32)
    return dict(noise=noise, stress=stress, timescale=timescale, mean_inflow=mean_inflow, courant=courant, prior_state=prior_state, field=field)


def filter_taps():
    offsets = jnp.arange(-FW, FW + 1).astype(jnp.float32)
    raw = jnp.exp(-math.pi * offsets * offsets / (2.0 * LS * LS))
    return (raw / jnp.sqrt(jnp.sum(raw * raw))).astype(jnp.bfloat16)

def cholesky_cells(stress):
    first_diag = jnp.sqrt(stress[0])
    second_low = stress[1] / first_diag
    second_diag = jnp.sqrt(stress[2] - second_low * second_low)
    third_low = stress[3] / first_diag
    third_mid = (stress[4] - second_low * third_low) / second_diag
    third_diag = jnp.sqrt(stress[5] - third_low * third_low - third_mid * third_mid)
    return (first_diag, second_low, second_diag, third_low, third_mid, third_diag)

def velocity_of(state, factors, mean_inflow):
    first_diag, second_low, second_diag, third_low, third_mid, third_diag = factors
    return jnp.stack([mean_inflow + first_diag * state[0], second_low * state[0] + second_diag * state[1], third_low * state[0] + third_mid * state[1] + third_diag * state[2]])

def march(current, courant, velocity):
    upstream = jnp.concatenate([velocity[:, None], current[:, :-1]], axis=1)
    return (1.0 - courant) * current + courant * upstream

def reference(noise, stress, timescale, mean_inflow, courant, prior_state, field):
    taps = filter_taps().astype(jnp.float32)
    decay = jnp.exp(-math.pi / (2.0 * timescale))
    gain = jnp.sqrt(1.0 - decay * decay)
    factors = cholesky_cells(stress)

    def one_plane(carry, plane):
        state, current = carry
        span = jnp.zeros(plane.shape, jnp.float32)
        for offset in range(2 * FW + 1):
            span = span + taps[offset] * jnp.roll(plane, FW - offset, axis=2).astype(jnp.float32)
        rounded = lax.optimization_barrier(span.astype(jnp.bfloat16))
        padded = jnp.pad(rounded, ((0, 0), (FW, FW), (0, 0))).astype(jnp.float32)
        filtered = jnp.zeros(plane.shape, jnp.float32)
        for offset in range(2 * FW + 1):
            filtered = filtered + taps[offset] * padded[:, offset:offset + NY, :]
        state = decay * state + gain * jnp.swapaxes(filtered, 1, 2)
        velocity = velocity_of(state, factors, mean_inflow)
        current = march(current, courant, velocity)
        return ((state, current), velocity.astype(jnp.bfloat16))
    (state, current), inflow = lax.scan(one_plane, (prior_state, field), noise)
    return (inflow, current)
```

```python
import functools
import math

import jax
import jax.numpy as jnp
import ml_dtypes
import numpy as np
from jax import lax
from jax.experimental import pallas as pl
from jax.experimental.pallas import tpu as pltpu
from jax.sharding import PartitionSpec as P

LS = 2
FW = 4
MESH = pl.DeviceIdType.MESH
BF16 = jnp.bfloat16
F32 = jnp.float32

LANES = 128
ROWS = 16
ZB = 256


def filter_taps():
    offsets = np.arange(-FW, FW + 1).astype(np.float32)
    raw = np.exp(np.float32(-math.pi) * offsets * offsets / np.float32(2.0 * LS * LS))
    taps = raw / np.sqrt(np.sum(raw * raw, dtype=np.float32))
    return [float(v) for v in taps.astype(ml_dtypes.bfloat16).astype(np.float32)]


def iota(shape, dim):
    return lax.broadcasted_iota(jnp.int32, shape, dim)


def banded(distance, keep):
    value = jnp.zeros(distance.shape, F32)
    for i, tap in enumerate(filter_taps()):
        value = jnp.where(distance == i - FW, tap, value)
    if keep is not None:
        value = jnp.where(keep, value, 0.0)
    return value.astype(BF16)


def kernel(
    cfg,
    noise_h, stress_h, time_h, mean_h, courant_h, prior_h, field_h,
    inflow_ref, out_ref,
    nz, stress, timescale, mean, courant, prior, field,
    wz, wy, sel, unsel, sent, sent_halo, got, got_halo, filt, velo,
    noise_sem, in_sem, send_sem, recv_sem, halo_send_sem, halo_recv_sem,
):
    G, dims = cfg["groups"], cfg["dims"]
    TN = dims[0] * dims[1] * dims[2]
    S = TN // G
    planes, comps, band, NZ = noise_h.shape
    depth = field_h.shape[1]
    chunks = got.shape[0]
    pairs = comps * planes // 2
    msg = pairs * ROWS
    g, t = lax.axis_index("grp"), lax.axis_index("tile")
    home = t // S
    place = t % S
    is_self = home == g
    has_low, has_high = g > 0, g < G - 1
    edge_low = jnp.logical_and(place == 0, home > 0)
    edge_high = jnp.logical_and(place == S - 1, home < G - 1)

    barrier = pltpu.get_barrier_semaphore()

    def greet(tile):
        def one(h, _):
            @pl.when(jnp.logical_not(jnp.logical_and(h == g, tile == t)))
            def _():
                pl.semaphore_signal(barrier, inc=1, device_id=(h, tile), device_id_type=MESH)
            return 0
        lax.fori_loop(0, G, one, 0)

    def greet_all(s, _):
        greet(g * S + s)
        return 0

    zcopies = [
        pltpu.make_async_copy(noise_h, nz.at[:, :, :, pl.ds(LANES, NZ)], noise_sem.at[0]),
        pltpu.make_async_copy(noise_h.at[:, :, :, pl.ds(NZ - LANES, LANES)], nz.at[:, :, :, pl.ds(0, LANES)], noise_sem.at[1]),
        pltpu.make_async_copy(noise_h.at[:, :, :, pl.ds(0, LANES)], nz.at[:, :, :, pl.ds(LANES + NZ, LANES)], noise_sem.at[2]),
    ]
    for copy in zcopies:
        copy.start()
    others = [
        pltpu.make_async_copy(src, dst, in_sem.at[i])
        for i, (src, dst) in enumerate(
            [(stress_h, stress), (time_h, timescale), (mean_h, mean), (courant_h, courant), (prior_h, prior), (field_h, field)]
        )
    ]
    lax.fori_loop(0, S, greet_all, 0)
    pl.when(has_low)(lambda: greet(g * S - 1))
    pl.when(has_high)(lambda: greet(g * S + S))

    wz[...] = banded(iota(wz.shape, 1) - iota(wz.shape, 0) - LANES, None)
    for copy in zcopies:
        copy.wait()
    for copy in others:
        copy.start()

    per = ZB // 64

    def span_block(b, _):
        first = pl.multiple_of(b * ZB, ZB)
        for c in range(comps):
            rhs = nz[:, c, :, pl.ds(first, 2 * ZB)].reshape(planes * band, 2 * ZB)
            out = lax.dot_general(wz[...], rhs, (((1,), (1,)), ((), ())), preferred_element_type=F32)
            out = out.astype(BF16)
            for ph in range(planes // 2):
                part = out[:, ph * LANES:(ph + 1) * LANES].reshape(per, chunks, ROWS, LANES)
                for k in range(chunks):
                    sent[k, pl.ds(b * per, per), pl.ds((c * (planes // 2) + ph) * ROWS, ROWS), :] = part[:, k]
        return 0

    lax.fori_loop(0, NZ // ZB, span_block, 0)

    is_edge = jnp.logical_or(edge_low, edge_high)
    own_halo = jnp.logical_or(
        jnp.logical_and(edge_high, home + 1 == g), jnp.logical_and(edge_low, home - 1 == g)
    )
    one, none = jnp.int32(1), jnp.int32(0)
    expected = (
        TN - jnp.where(is_self, one, none)
        + jnp.where(is_edge, jnp.int32(TN), none)
        - jnp.where(own_halo, one, none)
    )
    pl.semaphore_wait(barrier, expected)

    tx, ty, tc = t // (dims[1] * dims[2]), (t // dims[2]) % dims[1], t % dims[2]

    def dest_tile(j):
        dx, dy, dc = j // (dims[1] * dims[2]), (j // dims[2]) % dims[1], j % dims[2]
        return (((tx + dx) % dims[0]) * dims[1] + (ty + dy) % dims[1]) * dims[2] + (tc + dc) % dims[2]

    my_slot = (place + 1) * G + g

    def send_chunk(k):
        def one(j, _):
            to = dest_tile(j)
            mine = jnp.logical_and(is_self, to == t)

            @pl.when(jnp.logical_not(mine))
            def _():
                pltpu.make_async_remote_copy(
                    sent.at[k, to], got.at[k, my_slot], send_sem.at[k], recv_sem.at[k],
                    device_id=(home, to), device_id_type=MESH,
                ).start()

            return 0

        lax.fori_loop(0, TN, one, 0)

        @pl.when(is_self)
        def _():
            got[k, my_slot] = sent[k, t]

    send_chunk(0)


    @pl.when(is_edge)
    def _():
        top = jnp.where(edge_high, band - FW, 0)
        half = LANES // 2
        for i in range(pairs):
            row, col = iota((LANES, half), 0), iota((LANES, half), 1)
            h, y = row // half, row % half
            hit = jnp.logical_and(col - i * 2 * FW - h * FW == y - top, jnp.logical_and(y >= top, y < top + FW))
            sel[pl.ds(i * LANES, LANES), :] = jnp.where(hit, 1.0, 0.0).astype(BF16)

        def pack(j, _):
            for kk in range(chunks // 2):
                sides = []
                for e in range(2):
                    lhs = jnp.concatenate(
                        [sent[2 * kk + e, pl.ds(j * 4, 4), pl.ds(i * ROWS, ROWS), :].reshape(4 * ROWS, LANES) for i in range(pairs)],
                        axis=1,
                    )
                    sides.append(jnp.dot(lhs, sel[...], preferred_element_type=F32))
                both = jnp.concatenate(sides, axis=1).astype(BF16)
                sent_halo[pl.ds(j * 4, 4), pl.ds(kk * ROWS, ROWS), :] = both.reshape(4, ROWS, LANES)
            return 0

        lax.fori_loop(0, TN // 4, pack, 0)
        to_group = jnp.where(edge_high, home + 1, home - 1)
        side = jnp.where(edge_high, 0, 1)

        def one(j, _):
            to = dest_tile(j)
            mine = jnp.logical_and(to_group == g, to == t)

            @pl.when(jnp.logical_not(mine))
            def _():
                pltpu.make_async_remote_copy(
                    sent_halo.at[to], got_halo.at[side, g], halo_send_sem, halo_recv_sem.at[side],
                    device_id=(to_group, to), device_id_type=MESH,
                ).start()

            @pl.when(mine)
            def _():
                got_halo[side, g] = sent_halo[t]

            return 0

        lax.fori_loop(0, TN, one, 0)

    for k in range(1, chunks):
        send_chunk(k)

    row, col = iota(wy.shape, 0), iota(wy.shape, 1)
    wy[...] = banded(
        (row // LANES - 1) * 64 + row % 64 - col % LANES,
        (row // 64) % 2 == col // LANES,
    )
    half = LANES // 2
    for side in range(2):
        top = band - FW if side == 0 else 0
        for i in range(pairs):
            row, col = iota((LANES, LANES), 0), iota((LANES, LANES), 1)
            h, y = col // half, col % half
            want = i * 2 * FW + h * FW + y - top
            for e in range(2):
                hit = jnp.logical_and(row == want + e * half, jnp.logical_and(y >= top, y < top + FW))
                unsel[side, e, :, pl.ds(i * LANES, LANES)] = jnp.where(hit, 1.0, 0.0).astype(BF16)
    for copy in others:
        copy.wait()

    for side, there in ((0, has_low), (1, has_high)):
        own = jnp.logical_and(edge_high, home + 1 == g) if side == 0 else jnp.logical_and(edge_low, home - 1 == g)
        slot = 0 if side == 0 else S + 1

        @pl.when(jnp.logical_and(there, own))
        def _():
            part = got_halo.at[side, pl.ds(0, G - 1)]
            pltpu.make_async_copy(part, part, halo_recv_sem.at[side]).wait()

        @pl.when(jnp.logical_and(there, jnp.logical_not(own)))
        def _():
            part = got_halo.at[side]
            pltpu.make_async_copy(part, part, halo_recv_sem.at[side]).wait()

        @pl.when(there)
        def _():
            for k in range(chunks):
                lhs = got_halo[side, :, pl.ds((k // 2) * ROWS, ROWS), :].reshape(G * ROWS, LANES)
                rows = jnp.dot(lhs, unsel[side, k % 2], preferred_element_type=F32).astype(BF16)
                for i in range(pairs):
                    got[k, pl.ds(slot * G, G), pl.ds(i * ROWS, ROWS), :] = rows[:, i * LANES:(i + 1) * LANES].reshape(G, ROWS, LANES)

        @pl.when(jnp.logical_not(there))
        def _():
            for k in range(chunks):
                got[k, pl.ds(slot * G, G)] = jnp.zeros((G, msg, LANES), BF16)

    def chunk(k, _):
        @pl.when(is_self)
        def _():
            part = got.at[k, pl.ds(G, S * G - 1)]
            pltpu.make_async_copy(part, part, recv_sem.at[k]).wait()

        @pl.when(jnp.logical_not(is_self))
        def _():
            part = got.at[k, pl.ds(G, S * G)]
            pltpu.make_async_copy(part, part, recv_sem.at[k]).wait()

        def cells(yb, _):
            lanes = pl.ds(pl.multiple_of(yb * LANES, LANES), LANES)
            for p4 in range(G):
                lhs = jnp.concatenate([got[k, (2 * yb + s) * G + p4] for s in range(4)], axis=1)
                filt[pl.ds(p4 * msg, msg), :] = jnp.dot(lhs, wy[...], preferred_element_type=F32)
            for half_rows in range(2):
                r0 = half_rows * 8
                zr = pl.ds(pl.multiple_of(k * ROWS + r0, 8), 8)
                decay = jnp.exp(-math.pi / (2.0 * timescale[zr, lanes]))
                gain = jnp.sqrt(1.0 - decay * decay)
                per_gain = 1.0 / gain
                r = [stress[i, zr, lanes] for i in range(6)]
                l11 = jnp.sqrt(r[0])
                l21 = r[1] / l11
                l22 = jnp.sqrt(r[2] - l21 * l21)
                l31 = r[3] / l11
                l32 = (r[4] - l21 * l31) / l22
                l33 = jnp.sqrt(r[5] - l31 * l31 - l32 * l32)
                l11, l21, l22, l31, l32, l33 = (v * gain for v in (l11, l21, l22, l31, l32, l33))
                state = [prior[c, zr, lanes] * per_gain for c in range(3)]
                mean_in = mean[zr, lanes]
                cou = courant[zr, lanes]
                stay = 1.0 - cou
                per_cou = 1.0 / cou
                current = []
                for c in range(3):
                    scale = per_cou
                    line = []
                    for x in range(depth):
                        line.append(field[c, x, zr, lanes] * scale)
                        scale = scale * per_cou
                    current.append(line)
                for p in range(planes * G):
                    at = [(p // planes) * msg + (c * (planes // 2) + (p % planes) // 2) * ROWS + r0 for c in range(3)]
                    side = (p % 2) * LANES
                    state = [decay * state[c] + filt[pl.ds(at[c], 8), pl.ds(side, LANES)] for c in range(3)]
                    vel = [
                        mean_in + l11 * state[0],
                        l21 * state[0] + l22 * state[1],
                        l31 * state[0] + l32 * state[1] + l33 * state[2],
                    ]
                    for c in range(3):
                        velo[p, c, pl.ds(r0, 8), :] = vel[c]
                        line = current[c]
                        current[c] = [stay * line[x] + (line[x - 1] if x else vel[c]) for x in range(depth)]
                for c in range(3):
                    scale = cou
                    for x in range(depth):
                        out_ref[c, x, zr, lanes] = current[c][x] * scale
                        scale = scale * cou
            zr = pl.ds(pl.multiple_of(k * ROWS, ROWS), ROWS)
            for p in range(planes * G):
                for c in range(3):
                    inflow_ref[p, c, zr, lanes] = velo[p, c].astype(BF16)
            return 0

        lax.fori_loop(0, inflow_ref.shape[3] // LANES, cells, 0)
        return 0

    lax.fori_loop(0, chunks, chunk, 0)

    def drain(k, _):
        @pl.when(is_self)
        def _():
            part = sent.at[k, pl.ds(0, TN - 1)]
            pltpu.make_async_copy(part, part, send_sem.at[k]).wait()

        @pl.when(jnp.logical_not(is_self))
        def _():
            part = sent.at[k]
            pltpu.make_async_copy(part, part, send_sem.at[k]).wait()

        return 0

    lax.fori_loop(0, chunks, drain, 0)

    @pl.when(jnp.logical_and(is_edge, own_halo))
    def _():
        part = sent_halo.at[pl.ds(0, TN - 1)]
        pltpu.make_async_copy(part, part, halo_send_sem).wait()

    @pl.when(jnp.logical_and(is_edge, jnp.logical_not(own_halo)))
    def _():
        pltpu.make_async_copy(sent_halo, sent_halo, halo_send_sem).wait()


def body(cfg, noise, stress, timescale, mean_inflow, courant, prior_state, field):
    G, dims = cfg["groups"], cfg["dims"]
    TN = dims[0] * dims[1] * dims[2]
    S = TN // G
    planes, comps, band, NZ = noise.shape
    depth, width, length = field.shape[1:]
    assert band == 64 and width == 64 and length == S * band and NZ == TN * width
    chunks = width // ROWS
    pairs = comps * planes // 2
    msg = pairs * ROWS
    hbm_spec = pl.BlockSpec(memory_space=pltpu.HBM)
    vmem_spec = pl.BlockSpec(memory_space=pltpu.VMEM)
    return pl.pallas_call(
        functools.partial(kernel, cfg),
        out_shape=(
            pltpu.VMEM((planes * G, comps, width, length), BF16),
            pltpu.VMEM((comps, depth, width, length), F32),
        ),
        in_specs=[hbm_spec] * 7,
        out_specs=(vmem_spec, vmem_spec),
        scratch_shapes=[
            pltpu.VMEM((planes, comps, band, NZ + 2 * LANES), BF16),
            pltpu.VMEM(stress.shape, F32),
            pltpu.VMEM(timescale.shape, F32),
            pltpu.VMEM(mean_inflow.shape, F32),
            pltpu.VMEM(courant.shape, F32),
            pltpu.VMEM(prior_state.shape, F32),
            pltpu.VMEM(field.shape, F32),
            pltpu.VMEM((ZB, 2 * ZB), BF16),
            pltpu.VMEM((4 * LANES, 2 * LANES), BF16),
            pltpu.VMEM((pairs * LANES, LANES // 2), BF16),
            pltpu.VMEM((2, 2, LANES, pairs * LANES), BF16),
            pltpu.VMEM((chunks, TN, msg, LANES), BF16),
            pltpu.VMEM((TN, chunks // 2 * ROWS, LANES), BF16),
            pltpu.VMEM((chunks, (S + 2) * G, msg, LANES), BF16),
            pltpu.VMEM((2, G, chunks // 2 * ROWS, LANES), BF16),
            pltpu.VMEM((G * msg, 2 * LANES), F32),
            pltpu.VMEM((planes * G, comps, ROWS, LANES), F32),
            pltpu.SemaphoreType.DMA((3,)),
            pltpu.SemaphoreType.DMA((6,)),
            pltpu.SemaphoreType.DMA((chunks,)),
            pltpu.SemaphoreType.DMA((chunks,)),
            pltpu.SemaphoreType.DMA,
            pltpu.SemaphoreType.DMA((2,)),
        ],
        compiler_params=pltpu.CompilerParams(
            collective_id=0, has_side_effects=True, vmem_limit_bytes=40 * 2**20
        ),
        name="inflow",
    )(*[
        pltpu.with_memory_space_constraint(v, pltpu.HBM)
        for v in (noise, stress, timescale, mean_inflow, courant, prior_state, field)
    ])


TILE_DIMS = {32: (4, 4, 2), 8: (2, 2, 2), 4: (2, 1, 2)}


def solution(mesh):
    cfg = dict(groups=mesh.shape["grp"], dims=TILE_DIMS[mesh.shape["tile"]])
    placed = (
        P("grp", None, "tile", None),
        P(None, "tile", "grp"),
        P("tile", "grp"),
        P("tile", "grp"),
        P("tile", "grp"),
        P(None, "tile", "grp"),
        P(None, None, "tile", "grp"),
    )
    return jax.shard_map(
        functools.partial(body, cfg),
        mesh=mesh,
        in_specs=placed,
        out_specs=(P(None, None, "tile", "grp"), P(None, None, "tile", "grp")),
        check_vma=False,
    )
```

```python
import functools
import math

import jax
import jax.numpy as jnp
import ml_dtypes
import numpy as np
from jax import lax
from jax.experimental import pallas as pl
from jax.experimental.pallas import tpu as pltpu
from jax.sharding import PartitionSpec as P

LS = 2
FW = 4
MESH = pl.DeviceIdType.MESH
BF16 = jnp.bfloat16
F32 = jnp.float32

LANES = 128
ROWS = 16
ZB = 256


def filter_taps():
    offsets = np.arange(-FW, FW + 1).astype(np.float32)
    raw = np.exp(np.float32(-math.pi) * offsets * offsets / np.float32(2.0 * LS * LS))
    taps = raw / np.sqrt(np.sum(raw * raw, dtype=np.float32))
    return [float(v) for v in taps.astype(ml_dtypes.bfloat16).astype(np.float32)]


def iota(shape, dim):
    return lax.broadcasted_iota(jnp.int32, shape, dim)


def banded(distance, keep):
    value = jnp.zeros(distance.shape, F32)
    for i, tap in enumerate(filter_taps()):
        value = jnp.where(distance == i - FW, tap, value)
    if keep is not None:
        value = jnp.where(keep, value, 0.0)
    return value.astype(BF16)


def kernel(
    cfg,
    noise_h, stress_h, time_h, mean_h, courant_h, prior_h, field_h,
    inflow_ref, out_ref,
    nz, factor, decay, mean, courant, prior, field,
    wz, wy, sel, unsel, sent, sent_halo, got, got_halo, filt, states,
    noise_sem, in_sem, send_sem, recv_sem, halo_send_sem, halo_recv_sem,
):
    G, dims = cfg["groups"], cfg["dims"]
    TN = dims[0] * dims[1] * dims[2]
    S = TN // G
    planes, comps, band, NZ = noise_h.shape
    depth, width, length = field_h.shape[1:]
    chunks = width // ROWS
    halves = planes // 2
    pairs = comps * halves
    half = LANES // 2
    g, t = lax.axis_index("grp"), lax.axis_index("tile")
    home, place = lax.div(t, S), lax.rem(t, S)
    is_self = home == g
    has_low, has_high = g > 0, g < G - 1
    edge_low = jnp.logical_and(place == 0, home > 0)
    edge_high = jnp.logical_and(place == S - 1, home < G - 1)
    is_edge = jnp.logical_or(edge_low, edge_high)
    own_halo = jnp.logical_or(
        jnp.logical_and(edge_high, home + 1 == g), jnp.logical_and(edge_low, home - 1 == g)
    )
    one, none = jnp.int32(1), jnp.int32(0)

    zcopies = [
        pltpu.make_async_copy(noise_h, nz.at[:, :, :, pl.ds(LANES, NZ)], noise_sem.at[0]),
        pltpu.make_async_copy(noise_h.at[:, :, :, pl.ds(NZ - LANES, LANES)], nz.at[:, :, :, pl.ds(0, LANES)], noise_sem.at[1]),
        pltpu.make_async_copy(noise_h.at[:, :, :, pl.ds(0, LANES)], nz.at[:, :, :, pl.ds(LANES + NZ, LANES)], noise_sem.at[2]),
    ]
    for copy in zcopies:
        copy.start()
    others = [
        pltpu.make_async_copy(src, dst, in_sem.at[i])
        for i, (src, dst) in enumerate(
            [(stress_h, factor), (time_h, decay), (mean_h, mean), (courant_h, courant), (prior_h, prior), (field_h, field)]
        )
    ]

    barrier = pltpu.get_barrier_semaphore()

    def greet(tile):
        def tell(h, _):
            @pl.when(jnp.logical_not(jnp.logical_and(h == g, tile == t)))
            def _():
                pl.semaphore_signal(barrier, inc=1, device_id=(h, tile), device_id_type=MESH)
            return 0
        lax.fori_loop(0, G, tell, 0)

    def greet_all(s, _):
        greet(g * S + s)
        return 0

    lax.fori_loop(0, S, greet_all, 0)
    pl.when(has_low)(lambda: greet(g * S - 1))
    pl.when(has_high)(lambda: greet(g * S + S))

    wz[...] = banded(iota(wz.shape, 1) - iota(wz.shape, 0) - LANES, None)

    @pl.when(is_edge)
    def _():
        top = jnp.where(edge_high, jnp.int32(band - FW), none)
        for i in range(pairs):
            row, col = iota((LANES, LANES), 0), iota((LANES, LANES), 1)
            h, y = row // half, row % half
            inside = jnp.logical_and(y >= top, y < top + FW)
            want = i * 2 * FW + h * FW + y - top
            for e in range(2):
                hit = jnp.logical_and(col == want + e * half, inside)
                sel[e, pl.ds(i * LANES, LANES), :] = jnp.where(hit, 1.0, 0.0).astype(BF16)

    for copy in zcopies:
        copy.wait()
    for copy in others:
        copy.start()

    per = ZB // width

    def span_block(b, _):
        first = pl.multiple_of(b * ZB, ZB)
        for c in range(comps):
            rhs = nz[:, c, :, pl.ds(first, 2 * ZB)].reshape(planes * band, 2 * ZB)
            out = lax.dot_general(wz[...], rhs, (((1,), (1,)), ((), ())), preferred_element_type=F32)
            out = out.astype(BF16)
            for ph in range(halves):
                part = out[:, ph * LANES:(ph + 1) * LANES].reshape(per, chunks, ROWS, LANES)
                for k in range(chunks):
                    sent[k * comps + c, pl.ds(b * per, per), pl.ds(ph * ROWS, ROWS), :] = part[:, k]
        return 0

    lax.fori_loop(0, NZ // ZB, span_block, 0)

    tx, ty, tc = lax.div(t, dims[1] * dims[2]), lax.rem(lax.div(t, dims[2]), dims[1]), lax.rem(t, dims[2])

    def dest_tile(j):
        dx, dy, dc = lax.div(j, dims[1] * dims[2]), lax.rem(lax.div(j, dims[2]), dims[1]), lax.rem(j, dims[2])
        return (lax.rem(tx + dx, dims[0]) * dims[1] + lax.rem(ty + dy, dims[1])) * dims[2] + lax.rem(tc + dc, dims[2])

    @pl.when(is_edge)
    def _():
        for kk in range(chunks // 2):
            total = None
            for e in range(2):
                lhs = jnp.concatenate(
                    [
                        sent[(2 * kk + e) * comps + i // halves, :, pl.ds((i % halves) * ROWS, ROWS), :].reshape(TN * ROWS, LANES)
                        for i in range(pairs)
                    ],
                    axis=1,
                )
                part = jnp.dot(lhs, sel[e], preferred_element_type=F32)
                total = part if total is None else total + part
            sent_halo[:, pl.ds(kk * ROWS, ROWS), :] = total.astype(BF16).reshape(TN, ROWS, LANES)

    expected = (
        TN - jnp.where(is_self, one, none)
        + jnp.where(is_edge, jnp.int32(TN), none)
        - jnp.where(own_halo, one, none)
    )
    pl.semaphore_wait(barrier, expected)

    @pl.when(is_edge)
    def _():
        to_group = jnp.where(edge_high, home + 1, home - 1)
        side = jnp.where(edge_high, none, one)

        def send(j, _):
            to = dest_tile(j)
            pltpu.make_async_remote_copy(
                sent_halo.at[to], got_halo.at[side, g], halo_send_sem, halo_recv_sem.at[side],
                device_id=(to_group, to), device_id_type=MESH,
            ).start()
            return 0

        lax.fori_loop(jnp.where(own_halo, one, none), TN, send, 0)

    my_slot = (place + 1) * G + g
    first_send = jnp.where(is_self, one, none)

    def send_chunk(q, _):
        def send(j, _):
            to = dest_tile(j)
            pltpu.make_async_remote_copy(
                sent.at[q, to], got.at[q, my_slot], send_sem.at[q], recv_sem.at[q],
                device_id=(home, to), device_id_type=MESH,
            ).start()
            return 0

        return lax.fori_loop(first_send, TN, send, 0)

    lax.fori_loop(0, chunks * comps, send_chunk, 0)

    @pl.when(is_self)
    def _():
        got[:, my_slot] = sent[:, t]

    @pl.when(own_halo)
    def _():
        side = jnp.where(edge_high, none, one)
        got_halo[side, g] = sent_halo[t]

    row, col = iota(wy.shape, 0), iota(wy.shape, 1)
    wy[...] = banded(
        (row // LANES - 1) * half + row % half - col % LANES,
        (row // half) % 2 == col // LANES,
    )
    for side in range(2):
        top = band - FW if side == 0 else 0
        for i in range(pairs):
            row, col = iota((LANES, LANES), 0), iota((LANES, LANES), 1)
            h, y = col // half, col % half
            want = i * 2 * FW + h * FW + y - top
            for e in range(2):
                hit = jnp.logical_and(row == want + e * half, jnp.logical_and(y >= top, y < top + FW))
                unsel[side, e, :, pl.ds(i * LANES, LANES)] = jnp.where(hit, 1.0, 0.0).astype(BF16)
    for copy in others:
        copy.wait()

    def prepare(n, _):
        zr = pl.ds(pl.multiple_of(lax.div(n, length // LANES) * ROWS, ROWS), ROWS)
        lanes = pl.ds(pl.multiple_of(lax.rem(n, length // LANES) * LANES, LANES), LANES)
        fade = jnp.exp(-math.pi / (2.0 * decay[zr, lanes]))
        gain = jnp.sqrt(1.0 - fade * fade)
        per_gain = 1.0 / gain
        r = [factor[i, zr, lanes] for i in range(6)]
        l11 = jnp.sqrt(r[0])
        l21 = r[1] / l11
        l22 = jnp.sqrt(r[2] - l21 * l21)
        l31 = r[3] / l11
        l32 = (r[4] - l21 * l31) / l22
        l33 = jnp.sqrt(r[5] - l31 * l31 - l32 * l32)
        for i, v in enumerate((l11, l21, l22, l31, l32, l33)):
            factor[i, zr, lanes] = v * gain
        decay[zr, lanes] = fade
        per_cou = 1.0 / courant[zr, lanes]
        for c in range(comps):
            prior[c, zr, lanes] = prior[c, zr, lanes] * per_gain
            scale = per_cou
            for x in range(depth):
                field[c, x, zr, lanes] = field[c, x, zr, lanes] * scale
                scale = scale * per_cou
        return 0

    lax.fori_loop(0, chunks * (length // LANES), prepare, 0)

    for side, there in ((0, has_low), (1, has_high)):
        own = jnp.logical_and(edge_high, home + 1 == g) if side == 0 else jnp.logical_and(edge_low, home - 1 == g)
        slot = 0 if side == 0 else S + 1

        @pl.when(jnp.logical_and(there, own))
        def _():
            part = got_halo.at[side, pl.ds(0, G - 1)]
            pltpu.make_async_copy(part, part, halo_recv_sem.at[side]).wait()

        @pl.when(jnp.logical_and(there, jnp.logical_not(own)))
        def _():
            part = got_halo.at[side]
            pltpu.make_async_copy(part, part, halo_recv_sem.at[side]).wait()

        @pl.when(there)
        def _():
            for k in range(chunks):
                lhs = got_halo[side, :, pl.ds((k // 2) * ROWS, ROWS), :].reshape(G * ROWS, LANES)
                rows = jnp.dot(lhs, unsel[side, k % 2], preferred_element_type=F32).astype(BF16)
                for i in range(pairs):
                    got[k * comps + i // halves, pl.ds(slot * G, G), pl.ds((i % halves) * ROWS, ROWS), :] = (
                        rows[:, i * LANES:(i + 1) * LANES].reshape(G, ROWS, LANES)
                    )

        @pl.when(jnp.logical_not(there))
        def _():
            for q in range(chunks * comps):
                got[q, pl.ds(slot * G, G)] = jnp.zeros((G, halves * ROWS, LANES), BF16)

    def chunk(k, _):
        zr = pl.ds(pl.multiple_of(k * ROWS, ROWS), ROWS)
        for c in range(comps):
            q = k * comps + c

            @pl.when(is_self)
            def _():
                part = got.at[q, pl.ds(G, S * G - 1)]
                pltpu.make_async_copy(part, part, recv_sem.at[q]).wait()

            @pl.when(jnp.logical_not(is_self))
            def _():
                part = got.at[q, pl.ds(G, S * G)]
                pltpu.make_async_copy(part, part, recv_sem.at[q]).wait()

            for yb in range(length // LANES):
                lhs = jnp.concatenate(
                    [got[q, pl.ds((2 * yb + s) * G, G)].reshape(G * halves * ROWS, LANES) for s in range(4)], axis=1
                )
                filt[yb] = jnp.dot(lhs, wy[...], preferred_element_type=F32)

            def cells(yb, _):
                lanes = pl.ds(pl.multiple_of(yb * LANES, LANES), LANES)
                fade = decay[zr, lanes]
                state = prior[c, zr, lanes]
                low = [factor[c * (c + 1) // 2 + i, zr, lanes] for i in range(c + 1)]
                cou = courant[zr, lanes]
                stay = 1.0 - cou
                line = [field[c, x, zr, lanes] for x in range(depth)]
                for p in range(planes * G):
                    at = ((p // planes) * halves + (p % planes) // 2) * ROWS
                    state = fade * state + filt[yb, pl.ds(at, ROWS), pl.ds((p % 2) * LANES, LANES)]
                    vel = low[c] * state
                    for i in range(c):
                        vel = vel + low[i] * states[i, yb, p]
                    if c == 0:
                        vel = vel + mean[zr, lanes]
                    if c < comps - 1:
                        states[c, yb, p] = state
                    inflow_ref[p, c, zr, lanes] = vel.astype(BF16)
                    line = [stay * line[x] + (line[x - 1] if x else vel) for x in range(depth)]
                scale = cou
                for x in range(depth):
                    out_ref[c, x, zr, lanes] = line[x] * scale
                    scale = scale * cou
                return 0

            lax.fori_loop(0, length // LANES, cells, 0)
        return 0

    lax.fori_loop(0, chunks, chunk, 0)

    def drain(q, _):
        @pl.when(is_self)
        def _():
            part = sent.at[q, pl.ds(0, TN - 1)]
            pltpu.make_async_copy(part, part, send_sem.at[q]).wait()

        @pl.when(jnp.logical_not(is_self))
        def _():
            part = sent.at[q]
            pltpu.make_async_copy(part, part, send_sem.at[q]).wait()

        return 0

    lax.fori_loop(0, chunks * comps, drain, 0)

    @pl.when(jnp.logical_and(is_edge, own_halo))
    def _():
        part = sent_halo.at[pl.ds(0, TN - 1)]
        pltpu.make_async_copy(part, part, halo_send_sem).wait()

    @pl.when(jnp.logical_and(is_edge, jnp.logical_not(own_halo)))
    def _():
        pltpu.make_async_copy(sent_halo, sent_halo, halo_send_sem).wait()


def body(cfg, noise, stress, timescale, mean_inflow, courant, prior_state, field):
    G, dims = cfg["groups"], cfg["dims"]
    TN = dims[0] * dims[1] * dims[2]
    S = TN // G
    planes, comps, band, NZ = noise.shape
    depth, width, length = field.shape[1:]
    assert band == 64 and width == 64 and length == S * band and NZ == TN * width
    chunks = width // ROWS
    pairs = comps * planes // 2
    halves = planes // 2
    cuts = chunks * comps
    hbm_spec = pl.BlockSpec(memory_space=pltpu.HBM)
    vmem_spec = pl.BlockSpec(memory_space=pltpu.VMEM)
    return pl.pallas_call(
        functools.partial(kernel, cfg),
        out_shape=(
            pltpu.VMEM((planes * G, comps, width, length), BF16),
            pltpu.VMEM((comps, depth, width, length), F32),
        ),
        in_specs=[hbm_spec] * 7,
        out_specs=(vmem_spec, vmem_spec),
        scratch_shapes=[
            pltpu.VMEM((planes, comps, band, NZ + 2 * LANES), BF16),
            pltpu.VMEM(stress.shape, F32),
            pltpu.VMEM(timescale.shape, F32),
            pltpu.VMEM(mean_inflow.shape, F32),
            pltpu.VMEM(courant.shape, F32),
            pltpu.VMEM(prior_state.shape, F32),
            pltpu.VMEM(field.shape, F32),
            pltpu.VMEM((ZB, 2 * ZB), BF16),
            pltpu.VMEM((4 * LANES, 2 * LANES), BF16),
            pltpu.VMEM((2, pairs * LANES, LANES), BF16),
            pltpu.VMEM((2, 2, LANES, pairs * LANES), BF16),
            pltpu.VMEM((cuts, TN, halves * ROWS, LANES), BF16),
            pltpu.VMEM((TN, chunks // 2 * ROWS, LANES), BF16),
            pltpu.VMEM((cuts, (S + 2) * G, halves * ROWS, LANES), BF16),
            pltpu.VMEM((2, G, chunks // 2 * ROWS, LANES), BF16),
            pltpu.VMEM((length // LANES, G * halves * ROWS, 2 * LANES), F32),
            pltpu.VMEM((comps - 1, length // LANES, planes * G, ROWS, LANES), F32),
            pltpu.SemaphoreType.DMA((3,)),
            pltpu.SemaphoreType.DMA((6,)),
            pltpu.SemaphoreType.DMA((cuts,)),
            pltpu.SemaphoreType.DMA((cuts,)),
            pltpu.SemaphoreType.DMA,
            pltpu.SemaphoreType.DMA((2,)),
        ],
        compiler_params=pltpu.CompilerParams(
            collective_id=0, has_side_effects=True, vmem_limit_bytes=40 * 2**20
        ),
        name="inflow",
    )(*[
        pltpu.with_memory_space_constraint(v, pltpu.HBM)
        for v in (noise, stress, timescale, mean_inflow, courant, prior_state, field)
    ])


TILE_DIMS = {32: (4, 4, 2), 8: (2, 2, 2), 4: (2, 1, 2)}


def solution(mesh):
    cfg = dict(groups=mesh.shape["grp"], dims=TILE_DIMS[mesh.shape["tile"]])
    placed = (
        P("grp", None, "tile", None),
        P(None, "tile", "grp"),
        P("tile", "grp"),
        P("tile", "grp"),
        P("tile", "grp"),
        P(None, "tile", "grp"),
        P(None, None, "tile", "grp"),
    )
    return jax.shard_map(
        functools.partial(body, cfg),
        mesh=mesh,
        in_specs=placed,
        out_specs=(P(None, None, "tile", "grp"), P(None, None, "tile", "grp")),
        check_vma=False,
    )
```

```python
import functools
import math

import jax
import jax.numpy as jnp
import ml_dtypes
import numpy as np
from jax import lax
from jax.experimental import pallas as pl
from jax.experimental.pallas import tpu as pltpu
from jax.sharding import PartitionSpec as P

LS = 2
FW = 4
MESH = pl.DeviceIdType.MESH
BF16 = jnp.bfloat16
F32 = jnp.float32

LANES = 128
ROWS = 16
ZB = 256
GROUP = 2


def filter_taps():
    offsets = np.arange(-FW, FW + 1).astype(np.float32)
    raw = np.exp(np.float32(-math.pi) * offsets * offsets / np.float32(2.0 * LS * LS))
    taps = raw / np.sqrt(np.sum(raw * raw, dtype=np.float32))
    return [float(v) for v in taps.astype(ml_dtypes.bfloat16).astype(np.float32)]


def iota(shape, dim):
    return lax.broadcasted_iota(jnp.int32, shape, dim)


def banded(distance, keep):
    value = jnp.zeros(distance.shape, F32)
    for i, tap in enumerate(filter_taps()):
        value = jnp.where(distance == i - FW, tap, value)
    if keep is not None:
        value = jnp.where(keep, value, 0.0)
    return value.astype(BF16)


def kernel(
    cfg,
    noise_h, stress_h, time_h, mean_h, courant_h, prior_h, field_h,
    inflow_ref, out_ref,
    nz, factor, decay, mean, courant, prior, field,
    rim, wz, wy, sel, unsel, sent, sent_halo, got, got_halo, filt, states,
    noise_sem, in_sem, send_sem, recv_sem, halo_send_sem, halo_recv_sem,
):
    G, dims = cfg["groups"], cfg["dims"]
    TN = dims[0] * dims[1] * dims[2]
    S = TN // G
    planes, comps, band, NZ = noise_h.shape
    depth, width, length = field_h.shape[1:]
    chunks = width // ROWS
    halves = planes // 2
    pairs = comps * halves
    half = LANES // 2
    g, t = lax.axis_index("grp"), lax.axis_index("tile")
    home, place = lax.div(t, S), lax.rem(t, S)
    is_self = home == g
    has_low, has_high = g > 0, g < G - 1
    edge_low = jnp.logical_and(place == 0, home > 0)
    edge_high = jnp.logical_and(place == S - 1, home < G - 1)
    is_edge = jnp.logical_or(edge_low, edge_high)
    own_halo = jnp.logical_or(
        jnp.logical_and(edge_high, home + 1 == g), jnp.logical_and(edge_low, home - 1 == g)
    )
    one, none = jnp.int32(1), jnp.int32(0)

    blocks, per = NZ // ZB, ZB // width
    zcopies = [
        pltpu.make_async_copy(noise_h.at[:, :, :, pl.ds(b * ZB, ZB)], nz.at[b], noise_sem.at[b])
        for b in range(blocks)
    ]
    for copy in zcopies:
        copy.start()
    others = [
        pltpu.make_async_copy(src, dst, in_sem.at[i])
        for i, (src, dst) in enumerate(
            [(stress_h, factor), (time_h, decay), (mean_h, mean), (courant_h, courant), (prior_h, prior), (field_h, field)]
        )
    ]

    barrier = pltpu.get_barrier_semaphore()

    def greet(tile):
        def tell(h, _):
            @pl.when(jnp.logical_not(jnp.logical_and(h == g, tile == t)))
            def _():
                pl.semaphore_signal(barrier, inc=1, device_id=(h, tile), device_id_type=MESH)
            return 0
        lax.fori_loop(0, G, tell, 0)

    def greet_all(s, _):
        greet(g * S + s)
        return 0

    lax.fori_loop(0, S, greet_all, 0)
    pl.when(has_low)(lambda: greet(g * S - 1))
    pl.when(has_high)(lambda: greet(g * S + S))

    wz[...] = banded(iota(wz.shape, 1) - iota(wz.shape, 0) + ROWS, None)

    @pl.when(is_edge)
    def _():
        top = jnp.where(edge_high, jnp.int32(band - FW), none)
        for i in range(pairs):
            row, col = iota((LANES, LANES), 0), iota((LANES, LANES), 1)
            h, y = row // half, row % half
            inside = jnp.logical_and(y >= top, y < top + FW)
            want = i * 2 * FW + h * FW + y - top
            for e in range(2):
                hit = jnp.logical_and(col == want + e * half, inside)
                sel[e, pl.ds(i * LANES, LANES), :] = jnp.where(hit, 1.0, 0.0).astype(BF16)

    def put(b, d, k, c, value):
        for ph in range(halves):
            sent[k * comps + c, b * per + d, pl.ds(ph * ROWS, ROWS), :] = (
                value[:, ph * LANES:(ph + 1) * LANES].astype(BF16)
            )

    last = ZB - ROWS
    for group in range(0, blocks, GROUP):
        these = range(group, min(group + GROUP, blocks))
        for b in these:
            zcopies[b].wait()
        for b in these:
            for c in range(comps):
                rhs = nz[b, :, c].reshape(planes * band, ZB)
                out = lax.dot_general(wz[...], rhs, (((1,), (1,)), ((), ())), preferred_element_type=F32)
                rim[b, c, 0] = out[:ROWS]
                rim[b, c, 1] = out[ROWS:2 * ROWS]
                rim[b, c, 2] = out[ROWS + last:ROWS + ZB]
                rim[b, c, 3] = out[ROWS + ZB:]
                for n in range(1, ZB // ROWS - 1):
                    put(b, n // chunks, n % chunks, c, out[(n + 1) * ROWS:(n + 2) * ROWS])
    for copy in others:
        copy.start()
    for b in range(blocks):
        for c in range(comps):
            put(b, 0, 0, c, rim[b, c, 1] + rim[(b - 1) % blocks, c, 3])
            put(b, per - 1, chunks - 1, c, rim[b, c, 2] + rim[(b + 1) % blocks, c, 0])

    tx, ty, tc = lax.div(t, dims[1] * dims[2]), lax.rem(lax.div(t, dims[2]), dims[1]), lax.rem(t, dims[2])

    def dest_tile(j):
        dy, dx, dc = lax.div(j, dims[0] * dims[2]), lax.rem(lax.div(j, dims[2]), dims[0]), lax.rem(j, dims[2])
        return (lax.rem(tx + dx, dims[0]) * dims[1] + lax.rem(ty + dy, dims[1])) * dims[2] + lax.rem(tc + dc, dims[2])

    @pl.when(is_edge)
    def _():
        for kk in range(chunks // 2):
            total = None
            for e in range(2):
                lhs = jnp.concatenate(
                    [
                        sent[(2 * kk + e) * comps + i // halves, :, pl.ds((i % halves) * ROWS, ROWS), :].reshape(TN * ROWS, LANES)
                        for i in range(pairs)
                    ],
                    axis=1,
                )
                part = jnp.dot(lhs, sel[e], preferred_element_type=F32)
                total = part if total is None else total + part
            sent_halo[:, pl.ds(kk * ROWS, ROWS), :] = total.astype(BF16).reshape(TN, ROWS, LANES)

    expected = (
        TN - jnp.where(is_self, one, none)
        + jnp.where(is_edge, jnp.int32(TN), none)
        - jnp.where(own_halo, one, none)
    )
    pl.semaphore_wait(barrier, expected)

    @pl.when(is_edge)
    def _():
        to_group = jnp.where(edge_high, home + 1, home - 1)
        side = jnp.where(edge_high, none, one)

        def send(j, _):
            to = dest_tile(j)
            pltpu.make_async_remote_copy(
                sent_halo.at[to], got_halo.at[side, g], halo_send_sem, halo_recv_sem.at[side],
                device_id=(to_group, to), device_id_type=MESH,
            ).start()
            return 0

        lax.fori_loop(jnp.where(own_halo, one, none), TN, send, 0)

    my_slot = (place + 1) * G + g
    first_send = jnp.where(is_self, one, none)

    def send_chunk(q, _):
        def send(j, _):
            to = dest_tile(j)
            pltpu.make_async_remote_copy(
                sent.at[q, to], got.at[q, my_slot], send_sem.at[q], recv_sem.at[q],
                device_id=(home, to), device_id_type=MESH,
            ).start()
            return 0

        return lax.fori_loop(first_send, TN, send, 0)

    lax.fori_loop(0, chunks * comps, send_chunk, 0)

    @pl.when(is_self)
    def _():
        got[:, my_slot] = sent[:, t]

    @pl.when(own_halo)
    def _():
        side = jnp.where(edge_high, none, one)
        got_halo[side, g] = sent_halo[t]

    row, col = iota(wy.shape, 0), iota(wy.shape, 1)
    wy[...] = banded(
        (row // LANES - 1) * half + row % half - col % LANES,
        (row // half) % 2 == col // LANES,
    )
    for side in range(2):
        top = band - FW if side == 0 else 0
        for i in range(pairs):
            row, col = iota((LANES, LANES), 0), iota((LANES, LANES), 1)
            h, y = col // half, col % half
            want = i * 2 * FW + h * FW + y - top
            for e in range(2):
                hit = jnp.logical_and(row == want + e * half, jnp.logical_and(y >= top, y < top + FW))
                unsel[side, e, :, pl.ds(i * LANES, LANES)] = jnp.where(hit, 1.0, 0.0).astype(BF16)
    for copy in others:
        copy.wait()

    def prepare(n, _):
        zr = pl.ds(pl.multiple_of(lax.div(n, length // LANES) * ROWS, ROWS), ROWS)
        lanes = pl.ds(pl.multiple_of(lax.rem(n, length // LANES) * LANES, LANES), LANES)
        fade = jnp.exp(-math.pi / (2.0 * decay[zr, lanes]))
        gain = jnp.sqrt(1.0 - fade * fade)
        per_gain = 1.0 / gain
        r = [factor[i, zr, lanes] for i in range(6)]
        l11 = jnp.sqrt(r[0])
        l21 = r[1] / l11
        l22 = jnp.sqrt(r[2] - l21 * l21)
        l31 = r[3] / l11
        l32 = (r[4] - l21 * l31) / l22
        l33 = jnp.sqrt(r[5] - l31 * l31 - l32 * l32)
        for i, v in enumerate((l11, l21, l22, l31, l32, l33)):
            factor[i, zr, lanes] = v * gain
        decay[zr, lanes] = fade
        per_cou = 1.0 / courant[zr, lanes]
        for c in range(comps):
            prior[c, zr, lanes] = prior[c, zr, lanes] * per_gain
            scale = per_cou
            for x in range(depth):
                field[c, x, zr, lanes] = field[c, x, zr, lanes] * scale
                scale = scale * per_cou
        return 0

    lax.fori_loop(0, chunks * (length // LANES), prepare, 0)

    for side, there in ((0, has_low), (1, has_high)):
        own = jnp.logical_and(edge_high, home + 1 == g) if side == 0 else jnp.logical_and(edge_low, home - 1 == g)
        slot = 0 if side == 0 else S + 1

        @pl.when(jnp.logical_and(there, own))
        def _():
            part = got_halo.at[side, pl.ds(0, G - 1)]
            pltpu.make_async_copy(part, part, halo_recv_sem.at[side]).wait()

        @pl.when(jnp.logical_and(there, jnp.logical_not(own)))
        def _():
            part = got_halo.at[side]
            pltpu.make_async_copy(part, part, halo_recv_sem.at[side]).wait()

        @pl.when(there)
        def _():
            for k in range(chunks):
                lhs = got_halo[side, :, pl.ds((k // 2) * ROWS, ROWS), :].reshape(G * ROWS, LANES)
                rows = jnp.dot(lhs, unsel[side, k % 2], preferred_element_type=F32).astype(BF16)
                for i in range(pairs):
                    got[k * comps + i // halves, pl.ds(slot * G, G), pl.ds((i % halves) * ROWS, ROWS), :] = (
                        rows[:, i * LANES:(i + 1) * LANES].reshape(G, ROWS, LANES)
                    )

        @pl.when(jnp.logical_not(there))
        def _():
            for q in range(chunks * comps):
                got[q, pl.ds(slot * G, G)] = jnp.zeros((G, halves * ROWS, LANES), BF16)

    def chunk(k, _):
        zr = pl.ds(pl.multiple_of(k * ROWS, ROWS), ROWS)
        for c in range(comps):
            q = k * comps + c

            @pl.when(is_self)
            def _():
                part = got.at[q, pl.ds(G, S * G - 1)]
                pltpu.make_async_copy(part, part, recv_sem.at[q]).wait()

            @pl.when(jnp.logical_not(is_self))
            def _():
                part = got.at[q, pl.ds(G, S * G)]
                pltpu.make_async_copy(part, part, recv_sem.at[q]).wait()

            for yb in range(length // LANES):
                lhs = jnp.concatenate(
                    [got[q, pl.ds((2 * yb + s) * G, G)].reshape(G * halves * ROWS, LANES) for s in range(4)], axis=1
                )
                filt[yb] = jnp.dot(lhs, wy[...], preferred_element_type=F32)

            def cells(yb, _):
                lanes = pl.ds(pl.multiple_of(yb * LANES, LANES), LANES)
                fade = decay[zr, lanes]
                state = prior[c, zr, lanes]
                low = [factor[c * (c + 1) // 2 + i, zr, lanes] for i in range(c + 1)]
                cou = courant[zr, lanes]
                stay = 1.0 - cou
                line = [field[c, x, zr, lanes] for x in range(depth)]
                for p in range(planes * G):
                    at = ((p // planes) * halves + (p % planes) // 2) * ROWS
                    state = fade * state + filt[yb, pl.ds(at, ROWS), pl.ds((p % 2) * LANES, LANES)]
                    vel = low[c] * state
                    for i in range(c):
                        vel = vel + low[i] * states[i, yb, p]
                    if c == 0:
                        vel = vel + mean[zr, lanes]
                    if c < comps - 1:
                        states[c, yb, p] = state
                    inflow_ref[p, c, zr, lanes] = vel.astype(BF16)
                    line = [stay * line[x] + (line[x - 1] if x else vel) for x in range(depth)]
                scale = cou
                for x in range(depth):
                    out_ref[c, x, zr, lanes] = line[x] * scale
                    scale = scale * cou
                return 0

            lax.fori_loop(0, length // LANES, cells, 0)
        return 0

    lax.fori_loop(0, chunks, chunk, 0)

    def drain(q, _):
        @pl.when(is_self)
        def _():
            part = sent.at[q, pl.ds(0, TN - 1)]
            pltpu.make_async_copy(part, part, send_sem.at[q]).wait()

        @pl.when(jnp.logical_not(is_self))
        def _():
            part = sent.at[q]
            pltpu.make_async_copy(part, part, send_sem.at[q]).wait()

        return 0

    lax.fori_loop(0, chunks * comps, drain, 0)

    @pl.when(jnp.logical_and(is_edge, own_halo))
    def _():
        part = sent_halo.at[pl.ds(0, TN - 1)]
        pltpu.make_async_copy(part, part, halo_send_sem).wait()

    @pl.when(jnp.logical_and(is_edge, jnp.logical_not(own_halo)))
    def _():
        pltpu.make_async_copy(sent_halo, sent_halo, halo_send_sem).wait()


def body(cfg, noise, stress, timescale, mean_inflow, courant, prior_state, field):
    G, dims = cfg["groups"], cfg["dims"]
    TN = dims[0] * dims[1] * dims[2]
    S = TN // G
    planes, comps, band, NZ = noise.shape
    depth, width, length = field.shape[1:]
    assert band == 64 and width == 64 and length == S * band and NZ == TN * width
    chunks = width // ROWS
    pairs = comps * planes // 2
    halves = planes // 2
    cuts = chunks * comps
    hbm_spec = pl.BlockSpec(memory_space=pltpu.HBM)
    vmem_spec = pl.BlockSpec(memory_space=pltpu.VMEM)
    inflow, out = pl.pallas_call(
        functools.partial(kernel, cfg),
        out_shape=(
            pltpu.VMEM((planes * G, comps, width, length), BF16),
            pltpu.VMEM((comps, depth, width, length), F32),
        ),
        in_specs=[hbm_spec] * 7,
        out_specs=(vmem_spec, vmem_spec),
        scratch_shapes=[
            pltpu.VMEM((NZ // ZB, planes, comps, band, ZB), BF16),
            pltpu.VMEM(stress.shape, F32),
            pltpu.VMEM(timescale.shape, F32),
            pltpu.VMEM(mean_inflow.shape, F32),
            pltpu.VMEM(courant.shape, F32),
            pltpu.VMEM(prior_state.shape, F32),
            pltpu.VMEM(field.shape, F32),
            pltpu.VMEM((NZ // ZB, comps, 4, ROWS, planes * band), F32),
            pltpu.VMEM((ZB + 2 * ROWS, ZB), BF16),
            pltpu.VMEM((4 * LANES, 2 * LANES), BF16),
            pltpu.VMEM((2, pairs * LANES, LANES), BF16),
            pltpu.VMEM((2, 2, LANES, pairs * LANES), BF16),
            pltpu.VMEM((cuts, TN, halves * ROWS, LANES), BF16),
            pltpu.VMEM((TN, chunks // 2 * ROWS, LANES), BF16),
            pltpu.VMEM((cuts, (S + 2) * G, halves * ROWS, LANES), BF16),
            pltpu.VMEM((2, G, chunks // 2 * ROWS, LANES), BF16),
            pltpu.VMEM((length // LANES, G * halves * ROWS, 2 * LANES), F32),
            pltpu.VMEM((comps - 1, length // LANES, planes * G, ROWS, LANES), F32),
            pltpu.SemaphoreType.DMA((NZ // ZB,)),
            pltpu.SemaphoreType.DMA((6,)),
            pltpu.SemaphoreType.DMA((cuts,)),
            pltpu.SemaphoreType.DMA((cuts,)),
            pltpu.SemaphoreType.DMA,
            pltpu.SemaphoreType.DMA((2,)),
        ],
        compiler_params=pltpu.CompilerParams(
            collective_id=0, has_side_effects=True, vmem_limit_bytes=40 * 2**20
        ),
        name="inflow",
    )(*[
        pltpu.with_memory_space_constraint(v, pltpu.HBM)
        for v in (noise, stress, timescale, mean_inflow, courant, prior_state, field)
    ])
    return flush(inflow, out)


def flush_kernel(inflow_v, out_v, inflow_h, out_h, sems):
    copies = [
        pltpu.make_async_copy(inflow_v.at[pl.ds(i * n, n)], inflow_h.at[pl.ds(i * n, n)], sems.at[i])
        for n in (inflow_h.shape[0] // 4,)
        for i in range(4)
    ] + [
        pltpu.make_async_copy(out_v.at[c], out_h.at[c], sems.at[4 + c]) for c in range(out_h.shape[0])
    ]
    for copy in copies:
        copy.start()
    for copy in copies:
        copy.wait()


def flush(inflow, out):
    any_spec = pl.BlockSpec(memory_space=pl.ANY)
    return pl.pallas_call(
        flush_kernel,
        out_shape=(
            jax.ShapeDtypeStruct(inflow.shape, inflow.dtype),
            jax.ShapeDtypeStruct(out.shape, out.dtype),
        ),
        in_specs=[any_spec] * 2,
        out_specs=(any_spec, any_spec),
        scratch_shapes=[pltpu.SemaphoreType.DMA((4 + out.shape[0],))],
        compiler_params=pltpu.CompilerParams(vmem_limit_bytes=40 * 2**20),
        name="flush",
    )(inflow, out)


TILE_DIMS = {32: (4, 4, 2), 8: (2, 2, 2), 4: (2, 1, 2)}


def solution(mesh):
    cfg = dict(groups=mesh.shape["grp"], dims=TILE_DIMS[mesh.shape["tile"]])
    placed = (
        P("grp", None, "tile", None),
        P(None, "tile", "grp"),
        P("tile", "grp"),
        P("tile", "grp"),
        P("tile", "grp"),
        P(None, "tile", "grp"),
        P(None, None, "tile", "grp"),
    )
    return jax.shard_map(
        functools.partial(body, cfg),
        mesh=mesh,
        in_specs=placed,
        out_specs=(P(None, None, "tile", "grp"), P(None, None, "tile", "grp")),
        check_vma=False,
    )
```

```python
import functools
import math

import jax
import jax.numpy as jnp
import ml_dtypes
import numpy as np
from jax import lax
from jax.experimental import pallas as pl
from jax.experimental.pallas import tpu as pltpu
from jax.sharding import PartitionSpec as P

LS = 2
FW = 4
MESH = pl.DeviceIdType.MESH
BF16 = jnp.bfloat16
F32 = jnp.float32

LANES = 128
ROWS = 16
ZB = 256
GROUP = 2


def filter_taps():
    offsets = np.arange(-FW, FW + 1).astype(np.float32)
    raw = np.exp(np.float32(-math.pi) * offsets * offsets / np.float32(2.0 * LS * LS))
    taps = raw / np.sqrt(np.sum(raw * raw, dtype=np.float32))
    return [float(v) for v in taps.astype(ml_dtypes.bfloat16).astype(np.float32)]


def iota(shape, dim):
    return lax.broadcasted_iota(jnp.int32, shape, dim)


def banded(distance, keep):
    value = jnp.zeros(distance.shape, F32)
    for i, tap in enumerate(filter_taps()):
        value = jnp.where(distance == i - FW, tap, value)
    if keep is not None:
        value = jnp.where(keep, value, 0.0)
    return value.astype(BF16)


def kernel(
    cfg,
    noise_h, stress_h, time_h, mean_h, courant_h, prior_h, field_h,
    inflow_ref, out_ref,
    nz, factor, decay, mean, courant, prior, field,
    rim, wz, wy, sel, unsel, sent, sent_halo, got, got_halo, filt, states,
    noise_sem, in_sem, send_sem, recv_sem, halo_send_sem, halo_recv_sem,
):
    G, dims = cfg["groups"], cfg["dims"]
    TN = dims[0] * dims[1] * dims[2]
    S = TN // G
    planes, comps, band, NZ = noise_h.shape
    depth, width, length = field_h.shape[1:]
    chunks = width // ROWS
    halves = planes // 2
    pairs = comps * halves
    half = LANES // 2
    g, t = lax.axis_index("grp"), lax.axis_index("tile")
    home, place = lax.div(t, S), lax.rem(t, S)
    is_self = home == g
    has_low, has_high = g > 0, g < G - 1
    edge_low = jnp.logical_and(place == 0, home > 0)
    edge_high = jnp.logical_and(place == S - 1, home < G - 1)
    is_edge = jnp.logical_or(edge_low, edge_high)
    own_halo = jnp.logical_or(
        jnp.logical_and(edge_high, home + 1 == g), jnp.logical_and(edge_low, home - 1 == g)
    )
    one, none = jnp.int32(1), jnp.int32(0)

    blocks, per = NZ // ZB, ZB // width
    zcopies = [
        pltpu.make_async_copy(noise_h.at[:, :, :, pl.ds(b * ZB, ZB)], nz.at[b], noise_sem.at[b])
        for b in range(blocks)
    ]
    for copy in zcopies:
        copy.start()
    others = [
        pltpu.make_async_copy(src, dst, in_sem.at[i])
        for i, (src, dst) in enumerate(
            [(stress_h, factor), (time_h, decay), (mean_h, mean), (courant_h, courant), (prior_h, prior), (field_h, field)]
        )
    ]

    barrier = pltpu.get_barrier_semaphore()

    def greet(tile):
        def tell(h, _):
            @pl.when(jnp.logical_not(jnp.logical_and(h == g, tile == t)))
            def _():
                pl.semaphore_signal(barrier, inc=1, device_id=(h, tile), device_id_type=MESH)
            return 0
        lax.fori_loop(0, G, tell, 0)

    def greet_all(s, _):
        greet(g * S + s)
        return 0

    lax.fori_loop(0, S, greet_all, 0)
    pl.when(has_low)(lambda: greet(g * S - 1))
    pl.when(has_high)(lambda: greet(g * S + S))

    wz[...] = banded(iota(wz.shape, 1) - iota(wz.shape, 0) + ROWS, None)

    @pl.when(is_edge)
    def _():
        top = jnp.where(edge_high, jnp.int32(band - FW), none)
        for i in range(pairs):
            row, col = iota((LANES, LANES), 0), iota((LANES, LANES), 1)
            h, y = row // half, row % half
            inside = jnp.logical_and(y >= top, y < top + FW)
            want = i * 2 * FW + h * FW + y - top
            for e in range(2):
                hit = jnp.logical_and(col == want + e * half, inside)
                sel[e, pl.ds(i * LANES, LANES), :] = jnp.where(hit, 1.0, 0.0).astype(BF16)

    def put(b, d, k, c, value):
        for ph in range(halves):
            sent[k * comps + c, b * per + d, pl.ds(ph * ROWS, ROWS), :] = (
                value[:, ph * LANES:(ph + 1) * LANES].astype(BF16)
            )

    last = ZB - ROWS
    for group in range(0, blocks, GROUP):
        these = range(group, min(group + GROUP, blocks))
        for b in these:
            zcopies[b].wait()
        for b in these:
            for c in range(comps):
                rhs = nz[b, :, c].reshape(planes * band, ZB)
                out = lax.dot_general(wz[...], rhs, (((1,), (1,)), ((), ())), preferred_element_type=F32)
                rim[b, c, 0] = out[:ROWS]
                rim[b, c, 1] = out[ROWS:2 * ROWS]
                rim[b, c, 2] = out[ROWS + last:ROWS + ZB]
                rim[b, c, 3] = out[ROWS + ZB:]
                for n in range(1, ZB // ROWS - 1):
                    put(b, n // chunks, n % chunks, c, out[(n + 1) * ROWS:(n + 2) * ROWS])
    for copy in others:
        copy.start()
    for b in range(blocks):
        for c in range(comps):
            put(b, 0, 0, c, rim[b, c, 1] + rim[(b - 1) % blocks, c, 3])
            put(b, per - 1, chunks - 1, c, rim[b, c, 2] + rim[(b + 1) % blocks, c, 0])

    tx, ty, tc = lax.div(t, dims[1] * dims[2]), lax.rem(lax.div(t, dims[2]), dims[1]), lax.rem(t, dims[2])

    def dest_tile(j):
        dy, dx, dc = lax.div(j, dims[0] * dims[2]), lax.rem(lax.div(j, dims[2]), dims[0]), lax.rem(j, dims[2])
        return (lax.rem(tx + dx, dims[0]) * dims[1] + lax.rem(ty + dy, dims[1])) * dims[2] + lax.rem(tc + dc, dims[2])

    @pl.when(is_edge)
    def _():
        for kk in range(chunks // 2):
            total = None
            for e in range(2):
                lhs = jnp.concatenate(
                    [
                        sent[(2 * kk + e) * comps + i // halves, :, pl.ds((i % halves) * ROWS, ROWS), :].reshape(TN * ROWS, LANES)
                        for i in range(pairs)
                    ],
                    axis=1,
                )
                part = jnp.dot(lhs, sel[e], preferred_element_type=F32)
                total = part if total is None else total + part
            sent_halo[:, pl.ds(kk * ROWS, ROWS), :] = total.astype(BF16).reshape(TN, ROWS, LANES)

    expected = (
        TN - jnp.where(is_self, one, none)
        + jnp.where(is_edge, jnp.int32(TN), none)
        - jnp.where(own_halo, one, none)
    )
    pl.semaphore_wait(barrier, expected)

    @pl.when(is_edge)
    def _():
        to_group = jnp.where(edge_high, home + 1, home - 1)
        side = jnp.where(edge_high, none, one)

        def send(j, _):
            to = dest_tile(j)
            pltpu.make_async_remote_copy(
                sent_halo.at[to], got_halo.at[side, g], halo_send_sem, halo_recv_sem.at[side],
                device_id=(to_group, to), device_id_type=MESH,
            ).start()
            return 0

        lax.fori_loop(jnp.where(own_halo, one, none), TN, send, 0)

    my_slot = (place + 1) * G + g
    first_send = jnp.where(is_self, one, none)

    def send_chunk(q, _):
        def send(j, _):
            to = dest_tile(j)
            pltpu.make_async_remote_copy(
                sent.at[q, to], got.at[q, my_slot], send_sem.at[q], recv_sem.at[q],
                device_id=(home, to), device_id_type=MESH,
            ).start()
            return 0

        return lax.fori_loop(first_send, TN, send, 0)

    send_chunk(0, 0)

    row, col = iota(wy.shape, 0), iota(wy.shape, 1)
    wy[...] = banded(
        (row // LANES - 1) * half + row % half - col % LANES,
        (row // half) % 2 == col // LANES,
    )
    for side in range(2):
        top = band - FW if side == 0 else 0
        for i in range(pairs):
            row, col = iota((LANES, LANES), 0), iota((LANES, LANES), 1)
            h, y = col // half, col % half
            want = i * 2 * FW + h * FW + y - top
            for e in range(2):
                hit = jnp.logical_and(row == want + e * half, jnp.logical_and(y >= top, y < top + FW))
                unsel[side, e, :, pl.ds(i * LANES, LANES)] = jnp.where(hit, 1.0, 0.0).astype(BF16)
    lax.fori_loop(1, chunks * comps, send_chunk, 0)

    @pl.when(is_self)
    def _():
        got[:, my_slot] = sent[:, t]

    @pl.when(own_halo)
    def _():
        side = jnp.where(edge_high, none, one)
        got_halo[side, g] = sent_halo[t]

    for copy in others:
        copy.wait()

    def prepare(n, _):
        zr = pl.ds(pl.multiple_of(lax.div(n, length // LANES) * ROWS, ROWS), ROWS)
        lanes = pl.ds(pl.multiple_of(lax.rem(n, length // LANES) * LANES, LANES), LANES)
        fade = jnp.exp(-math.pi / (2.0 * decay[zr, lanes]))
        gain = jnp.sqrt(1.0 - fade * fade)
        per_gain = 1.0 / gain
        r = [factor[i, zr, lanes] for i in range(6)]
        l11 = jnp.sqrt(r[0])
        l21 = r[1] / l11
        l22 = jnp.sqrt(r[2] - l21 * l21)
        l31 = r[3] / l11
        l32 = (r[4] - l21 * l31) / l22
        l33 = jnp.sqrt(r[5] - l31 * l31 - l32 * l32)
        for i, v in enumerate((l11, l21, l22, l31, l32, l33)):
            factor[i, zr, lanes] = v * gain
        decay[zr, lanes] = fade
        per_cou = 1.0 / courant[zr, lanes]
        for c in range(comps):
            prior[c, zr, lanes] = prior[c, zr, lanes] * per_gain
            scale = per_cou
            for x in range(depth):
                field[c, x, zr, lanes] = field[c, x, zr, lanes] * scale
                scale = scale * per_cou
        return 0

    lax.fori_loop(0, chunks * (length // LANES), prepare, 0)

    for side, there in ((0, has_low), (1, has_high)):
        own = jnp.logical_and(edge_high, home + 1 == g) if side == 0 else jnp.logical_and(edge_low, home - 1 == g)
        slot = 0 if side == 0 else S + 1

        @pl.when(jnp.logical_and(there, own))
        def _():
            part = got_halo.at[side, pl.ds(0, G - 1)]
            pltpu.make_async_copy(part, part, halo_recv_sem.at[side]).wait()

        @pl.when(jnp.logical_and(there, jnp.logical_not(own)))
        def _():
            part = got_halo.at[side]
            pltpu.make_async_copy(part, part, halo_recv_sem.at[side]).wait()

        @pl.when(there)
        def _():
            for k in range(chunks):
                lhs = got_halo[side, :, pl.ds((k // 2) * ROWS, ROWS), :].reshape(G * ROWS, LANES)
                rows = jnp.dot(lhs, unsel[side, k % 2], preferred_element_type=F32).astype(BF16)
                for i in range(pairs):
                    got[k * comps + i // halves, pl.ds(slot * G, G), pl.ds((i % halves) * ROWS, ROWS), :] = (
                        rows[:, i * LANES:(i + 1) * LANES].reshape(G, ROWS, LANES)
                    )

        @pl.when(jnp.logical_not(there))
        def _():
            for q in range(chunks * comps):
                got[q, pl.ds(slot * G, G)] = jnp.zeros((G, halves * ROWS, LANES), BF16)

    def chunk(k, _):
        zr = pl.ds(pl.multiple_of(k * ROWS, ROWS), ROWS)
        for c in range(comps):
            q = k * comps + c

            @pl.when(is_self)
            def _():
                part = got.at[q, pl.ds(G, S * G - 1)]
                pltpu.make_async_copy(part, part, recv_sem.at[q]).wait()

            @pl.when(jnp.logical_not(is_self))
            def _():
                part = got.at[q, pl.ds(G, S * G)]
                pltpu.make_async_copy(part, part, recv_sem.at[q]).wait()

            for yb in range(length // LANES):
                lhs = jnp.concatenate(
                    [got[q, pl.ds((2 * yb + s) * G, G)].reshape(G * halves * ROWS, LANES) for s in range(4)], axis=1
                )
                filt[yb] = jnp.dot(lhs, wy[...], preferred_element_type=F32)

            def cells(yb, _):
                lanes = pl.ds(pl.multiple_of(yb * LANES, LANES), LANES)
                fade = decay[zr, lanes]
                state = prior[c, zr, lanes]
                low = [factor[c * (c + 1) // 2 + i, zr, lanes] for i in range(c + 1)]
                cou = courant[zr, lanes]
                stay = 1.0 - cou
                line = [field[c, x, zr, lanes] for x in range(depth)]
                for p in range(planes * G):
                    at = ((p // planes) * halves + (p % planes) // 2) * ROWS
                    state = fade * state + filt[yb, pl.ds(at, ROWS), pl.ds((p % 2) * LANES, LANES)]
                    vel = low[c] * state
                    for i in range(c):
                        vel = vel + low[i] * states[i, yb, p]
                    if c == 0:
                        vel = vel + mean[zr, lanes]
                    if c < comps - 1:
                        states[c, yb, p] = state
                    inflow_ref[p, c, zr, lanes] = vel.astype(BF16)
                    line = [stay * line[x] + (line[x - 1] if x else vel) for x in range(depth)]
                scale = cou
                for x in range(depth):
                    out_ref[c, x, zr, lanes] = line[x] * scale
                    scale = scale * cou
                return 0

            lax.fori_loop(0, length // LANES, cells, 0)
        return 0

    lax.fori_loop(0, chunks, chunk, 0)

    def drain(q, _):
        @pl.when(is_self)
        def _():
            part = sent.at[q, pl.ds(0, TN - 1)]
            pltpu.make_async_copy(part, part, send_sem.at[q]).wait()

        @pl.when(jnp.logical_not(is_self))
        def _():
            part = sent.at[q]
            pltpu.make_async_copy(part, part, send_sem.at[q]).wait()

        return 0

    lax.fori_loop(0, chunks * comps, drain, 0)

    @pl.when(jnp.logical_and(is_edge, own_halo))
    def _():
        part = sent_halo.at[pl.ds(0, TN - 1)]
        pltpu.make_async_copy(part, part, halo_send_sem).wait()

    @pl.when(jnp.logical_and(is_edge, jnp.logical_not(own_halo)))
    def _():
        pltpu.make_async_copy(sent_halo, sent_halo, halo_send_sem).wait()


def body(cfg, noise, stress, timescale, mean_inflow, courant, prior_state, field):
    G, dims = cfg["groups"], cfg["dims"]
    TN = dims[0] * dims[1] * dims[2]
    S = TN // G
    planes, comps, band, NZ = noise.shape
    depth, width, length = field.shape[1:]
    assert band == 64 and width == 64 and length == S * band and NZ == TN * width
    chunks = width // ROWS
    pairs = comps * planes // 2
    halves = planes // 2
    cuts = chunks * comps
    hbm_spec = pl.BlockSpec(memory_space=pltpu.HBM)
    vmem_spec = pl.BlockSpec(memory_space=pltpu.VMEM)
    inflow, out = pl.pallas_call(
        functools.partial(kernel, cfg),
        out_shape=(
            pltpu.VMEM((planes * G, comps, width, length), BF16),
            pltpu.VMEM((comps, depth, width, length), F32),
        ),
        in_specs=[hbm_spec] * 7,
        out_specs=(vmem_spec, vmem_spec),
        scratch_shapes=[
            pltpu.VMEM((NZ // ZB, planes, comps, band, ZB), BF16),
            pltpu.VMEM(stress.shape, F32),
            pltpu.VMEM(timescale.shape, F32),
            pltpu.VMEM(mean_inflow.shape, F32),
            pltpu.VMEM(courant.shape, F32),
            pltpu.VMEM(prior_state.shape, F32),
            pltpu.VMEM(field.shape, F32),
            pltpu.VMEM((NZ // ZB, comps, 4, ROWS, planes * band), F32),
            pltpu.VMEM((ZB + 2 * ROWS, ZB), BF16),
            pltpu.VMEM((4 * LANES, 2 * LANES), BF16),
            pltpu.VMEM((2, pairs * LANES, LANES), BF16),
            pltpu.VMEM((2, 2, LANES, pairs * LANES), BF16),
            pltpu.VMEM((cuts, TN, halves * ROWS, LANES), BF16),
            pltpu.VMEM((TN, chunks // 2 * ROWS, LANES), BF16),
            pltpu.VMEM((cuts, (S + 2) * G, halves * ROWS, LANES), BF16),
            pltpu.VMEM((2, G, chunks // 2 * ROWS, LANES), BF16),
            pltpu.VMEM((length // LANES, G * halves * ROWS, 2 * LANES), F32),
            pltpu.VMEM((comps - 1, length // LANES, planes * G, ROWS, LANES), F32),
            pltpu.SemaphoreType.DMA((NZ // ZB,)),
            pltpu.SemaphoreType.DMA((6,)),
            pltpu.SemaphoreType.DMA((cuts,)),
            pltpu.SemaphoreType.DMA((cuts,)),
            pltpu.SemaphoreType.DMA,
            pltpu.SemaphoreType.DMA((2,)),
        ],
        compiler_params=pltpu.CompilerParams(
            collective_id=0, has_side_effects=True, vmem_limit_bytes=40 * 2**20
        ),
        name="inflow",
    )(*[
        pltpu.with_memory_space_constraint(v, pltpu.HBM)
        for v in (noise, stress, timescale, mean_inflow, courant, prior_state, field)
    ])
    return flush(inflow, out)


def flush_kernel(inflow_v, out_v, inflow_h, out_h, sems):
    copies = [
        pltpu.make_async_copy(inflow_v.at[pl.ds(i * n, n)], inflow_h.at[pl.ds(i * n, n)], sems.at[i])
        for n in (inflow_h.shape[0] // 4,)
        for i in range(4)
    ] + [
        pltpu.make_async_copy(out_v.at[c], out_h.at[c], sems.at[4 + c]) for c in range(out_h.shape[0])
    ]
    for copy in copies:
        copy.start()
    for copy in copies:
        copy.wait()


def flush(inflow, out):
    any_spec = pl.BlockSpec(memory_space=pl.ANY)
    return pl.pallas_call(
        flush_kernel,
        out_shape=(
            jax.ShapeDtypeStruct(inflow.shape, inflow.dtype),
            jax.ShapeDtypeStruct(out.shape, out.dtype),
        ),
        in_specs=[any_spec] * 2,
        out_specs=(any_spec, any_spec),
        scratch_shapes=[pltpu.SemaphoreType.DMA((4 + out.shape[0],))],
        compiler_params=pltpu.CompilerParams(vmem_limit_bytes=40 * 2**20),
        name="flush",
    )(inflow, out)


TILE_DIMS = {32: (4, 4, 2), 8: (2, 2, 2), 4: (2, 1, 2)}


def solution(mesh):
    cfg = dict(groups=mesh.shape["grp"], dims=TILE_DIMS[mesh.shape["tile"]])
    placed = (
        P("grp", None, "tile", None),
        P(None, "tile", "grp"),
        P("tile", "grp"),
        P("tile", "grp"),
        P("tile", "grp"),
        P(None, "tile", "grp"),
        P(None, None, "tile", "grp"),
    )
    return jax.shard_map(
        functools.partial(body, cfg),
        mesh=mesh,
        in_specs=placed,
        out_specs=(P(None, None, "tile", "grp"), P(None, None, "tile", "grp")),
        check_vma=False,
    )
```
